128 devices in a mesh: slab: 32 (over z, x, core), rhs: 4 (over y).
Axes of the slice: x: 4, y: 4, z: 4, core: 2. Of those that a mesh axis runs over, the one named last changes fastest.
Arguments:
- diag_blocks: float32 [32, 512, 512], P('slab'), may hold values from -1 to 2, as said below
- sub_blocks: float32 [32, 512, 512], P('slab'), may hold values from -1 to 1
- right_side: float32 [256, 16384], P('rhs', 'slab'), may hold values from -6 to 6
- boundary: float32 [512, 256], P(None, 'rhs'), may hold values from -6 to 6
Outputs:
- solution: float32 [256, 16384], P('rhs', 'slab')
The draws below stay inside these ranges and needn't reach their ends.
Inputs may be any that keep to these rules, and one draw needn't show every extreme that they name: Each diag_blocks tile is lower triangular with diagonal entries from 0.8 to 1.25; each sub_blocks tile is upper triangular (zeros below its diagonal).
All inputs are finite; a program needn't handle non-finite values.
Results may differ from the reference program's by a relative error of at most 0.00021.
Values sent between devices are 32-bit elements; how exact they have to be, the bound alone decides.
No kernel may reach another device: no remote copies, remote signals or barrier semaphores. Data moves between devices by JAX's collectives and lax.ppermute only.
A program may use at most 64 MiB of HBM per device.

```python
import jax
import jax.numpy as jnp
from jax import lax

B = 512
NRHS = 256
TILE_DEV = 1
TILES = 32
ORDER = 16384
N_SLAB = 32


def draw_diag_blocks(key, part):
    first, second = jax.random.split(jax.random.fold_in(key, 11))
    lower_part = jax.random.normal(first, (TILE_DEV * N_SLAB, B, B), jnp.float32) * (0.3 / B ** 0.5)
    diag_vals = jax.random.uniform(second, (TILE_DEV * N_SLAB, B), jnp.float32, 0.8, 1.25)
    return jnp.tril(lower_part, -1) + jnp.eye(B, dtype=jnp.float32)[None, :, :] * diag_vals[:, None, :]


def draw_sub_blocks(key, part):
    base = jax.random.fold_in(key, 23)
    first, second, third, fourth, fifth = jax.random.split(base, 5)
    upper_part = jax.random.normal(first, (TILE_DEV * N_SLAB, B, B), jnp.float32) * (0.1 / B ** 0.5)
    slow_rate = jnp.exp(jnp.log(0.1) * jax.random.uniform(second, (B,), jnp.float32, 0.3, 1.0) / (TILE_DEV * N_SLAB))
    fast_rate = jax.random.uniform(third, (B,), jnp.float32, 0.2, 0.7)
    is_slow = jax.random.bernoulli(fourth, 0.5, (B,))
    signs = jnp.where(jax.random.bernoulli(fifth, 0.5, (B,)), 1.0, -1.0)
    diag_vals = signs * jnp.where(is_slow, slow_rate, fast_rate)
    return jnp.triu(upper_part, 1) + jnp.eye(B, dtype=jnp.float32)[None, :, :] * diag_vals[None, None, :]


def block_levels(rng, extent, shards, smallest, largest):
    def one(axis_at, blocks):
        draws = jax.random.uniform(jax.random.fold_in(jax.random.fold_in(rng, 6), axis_at), (blocks,), jnp.float32, smallest / len(shards), largest / len(shards))
        return jnp.repeat(jnp.exp(draws), extent[axis_at] // blocks).reshape((-1,) + (1,) * (len(extent) - axis_at - 1))

    factor_of = one(*shards[0])
    for cut in shards[1:]:
        factor_of = factor_of * one(*cut)
    return factor_of


def bell_draw(key, shape, spread, limit, shards=(), kind=jnp.bfloat16):
    values = spread * jax.random.normal(key, shape, jnp.float32)
    if shards:
        values = values * block_levels(key, shape, shards, -0.22, 0.18)
    return jnp.clip(values, -limit, limit).astype(kind)


def setup_inputs(seed: int = 0) -> dict:
    key_list = jax.random.split(jax.random.key(seed), 5)
    diag_blocks = draw_diag_blocks(jax.random.fold_in(key_list[4], 71), 0)
    sub_blocks = draw_sub_blocks(jax.random.fold_in(key_list[4], 71), 0)
    right_side = bell_draw(key_list[2], (NRHS, ORDER), 1.0, 6.0, ((0, 4), (1, 32)), jnp.float32)
    boundary = bell_draw(key_list[3], (B, NRHS), 1.0, 6.0, ((1, 4),), jnp.float32)
    return dict(diag_blocks=diag_blocks, sub_blocks=sub_blocks, right_side=right_side, boundary=boundary)


def reference(diag_blocks, sub_blocks, right_side, boundary):
    tiles_rhs = right_side.reshape(NRHS, TILES, B).transpose(1, 2, 0)

    def advance(previous, items):
        lower, upper, rhs_tile = items
        pushed = jnp.dot(upper, previous, precision=lax.Precision.HIGHEST)
        current = jax.scipy.linalg.solve_triangular(lower, rhs_tile - pushed, lower=True)
        return (current, current)
    final, solved = lax.scan(advance, boundary.astype(jnp.float32), (diag_blocks, sub_blocks, tiles_rhs))
    return solved.transpose(2, 0, 1).reshape(NRHS, ORDER)
```

```python
import functools

import jax
import jax.numpy as jnp
from jax import lax
from jax.experimental import pallas as pl
from jax.experimental.pallas import tpu as pltpu
from jax.sharding import Mesh
from jax.sharding import PartitionSpec as P

SLAB = ("z", "x", "c")
ALL = ("z", "x", "c", "y")
F32 = jnp.float32
BF16 = jnp.bfloat16
N = 512
H = 256
Q = 128
R = 64


def split(a):
    hi = a.astype(BF16)
    return hi, (a - hi.astype(F32)).astype(BF16)


def dot(a, b):
    return lax.dot_general(a, b, (((1,), (0,)), ((), ())), preferred_element_type=F32)


def mm(a, b):
    return dot(a[0], b[0]) + (dot(a[0], b[1]) + dot(a[1], b[0]))


def mm_small(a, b):
    ah, al = split(a)
    bh, bl = split(b)
    row = jnp.concatenate([bh, bl], axis=1)
    both = dot(jnp.concatenate([ah, al], axis=1), jnp.concatenate([row, row], axis=0))
    return both[:, :Q] + both[:, Q:]


def local_body(first_ref, diag_ref, sub_ref, right_ref, bound_ref, out_ref):
    row = lax.broadcasted_iota(jnp.int32, (Q, Q), 0)
    col = lax.broadcasted_iota(jnp.int32, (Q, Q), 1)
    eye = row == col

    def block(i, j):
        return diag_ref[0, j * Q:(j + 1) * Q, i * Q:(i + 1) * Q].T

    ups = [block(i, i) for i in range(4)]
    inv = []
    for u in ups:
        d = jnp.where(eye, u, 0.0)
        across = 1.0 / jnp.sum(d, axis=0, keepdims=True)
        down = 1.0 / jnp.sum(d, axis=1, keepdims=True)
        pair = ((row & 1) == 0) & (col == row + 1)
        inv.append(jnp.where(eye, across, jnp.where(pair, -(down * u) * across, 0.0)))
    for level in range(1, 7):
        rb, cb = row >> level, col >> level
        pick = ((rb & 1) == 0) & (cb == rb + 1)
        half = [mm_small(x, jnp.where(pick, u, 0.0)) for x, u in zip(inv, ups)]
        inv = [x - mm_small(h, x) for h, x in zip(half, inv)]
    tiles = []
    for i in (0, 2):
        off = mm_small(mm_small(inv[i], block(i, i + 1)), inv[i + 1])
        zero = jnp.zeros((Q, Q), F32)
        tiles.append(split(jnp.concatenate([
            jnp.concatenate([inv[i], -off], axis=1),
            jnp.concatenate([zero, inv[i + 1]], axis=1)], axis=0)))
    left0 = jnp.concatenate([sub_ref[0, :H, :].T, right_ref[:, :H]], axis=0)
    right0 = jnp.concatenate([sub_ref[0, H:, :].T, right_ref[:, H:]], axis=0)
    left = mm(split(left0), tiles[0])
    cross = split(diag_ref[0, H:, :H].T)
    right = mm(split(right0 - mm(split(left), cross)), tiles[1])
    out_ref[:N, :H] = -left[:N]
    out_ref[:N, H:] = -right[:N]
    out_ref[N:, :H] = left[N:]
    out_ref[N:, H:] = right[N:]

    @pl.when(first_ref[0] == 1)
    def _():
        out_ref[N:, :] += mm(split(bound_ref[...].T), split(out_ref[:N, :]))


def pair_body(core_ref, own_ref, other_ref, hi_ref, lo_ref, vec_ref):
    def go(first, second):
        both = mm(split(first[...]), split(second[:N, :]))
        hi, lo = split(both[:N])
        hi_ref[...] = hi
        lo_ref[...] = lo
        vec_ref[...] = both[N:] + second[N:, :]

    @pl.when(core_ref[0] == 0)
    def _():
        go(own_ref, other_ref)

    @pl.when(core_ref[0] == 1)
    def _():
        go(other_ref, own_ref)


def hop_body(got_ref, had_ref, hi_ref, lo_ref, vec_ref, in_ref, end_ref):
    total = had_ref[...] + got_ref[...]
    in_ref[...] = total
    end_ref[...] = vec_ref[...] + mm(split(total), (hi_ref[...], lo_ref[...]))


def last_body(core_ref, in_ref, end_ref, own_ref, out_ref):
    @pl.when(core_ref[0] == 0)
    def _():
        out_ref[...] = own_ref[N:, :] + mm(split(in_ref[...]), split(own_ref[:N, :]))

    @pl.when(core_ref[0] == 1)
    def _():
        out_ref[...] = end_ref[...]


def kernel(body, outs, name):
    smem = pl.BlockSpec(memory_space=pltpu.SMEM)
    vmem = pl.BlockSpec(memory_space=pltpu.VMEM)

    def call(*args):
        return pl.pallas_call(
            body,
            out_shape=outs,
            in_specs=[smem if a.dtype == jnp.int32 else vmem for a in args],
            out_specs=jax.tree.map(lambda _: vmem, outs),
            name=name,
        )(*args)

    return call


def arr(rows, dtype=F32):
    return jax.ShapeDtypeStruct((rows, N), dtype)


def index(z, x, c, y):
    return ((z * 4 + x) * 2 + c) * 4 + y


def local(diag_blocks, sub_blocks, right_side, boundary):
    core = lax.axis_index("c").astype(jnp.int32).reshape(1)
    first = (lax.axis_index(SLAB) == 0).astype(jnp.int32).reshape(1)
    own = kernel(local_body, arr(N + R), "local")(first, diag_blocks, sub_blocks, right_side, boundary)
    other = lax.ppermute(own, "c", [(0, 1), (1, 0)])
    hi, lo, vec = kernel(pair_body, [arr(N, BF16), arr(N, BF16), arr(R)], "pair")(core, own, other)
    inflow = jnp.zeros((R, N), F32)
    end = vec
    hop = kernel(hop_body, [arr(R), arr(R)], "hop")
    for k in range(15):
        pairs = [(index(k // 4, k % 4, 1, y), index((k + 1) // 4, (k + 1) % 4, 1, y)) for y in range(4)]
        got = lax.ppermute(end, ALL, pairs)
        inflow, end = hop(got, inflow, hi, lo, vec)
    chips = [(z, x, y) for z in range(4) for x in range(4) for y in range(4)]
    down = lax.ppermute(inflow, ALL, [(index(z, x, 1, y), index(z, x, 0, y)) for z, x, y in chips])
    return kernel(last_body, arr(R), "last")(core, down, end, own)


def solution(mesh):
    shape = mesh.devices.reshape(4, 4, 2, 4)
    split_mesh = Mesh(shape, ALL)
    placed = (P(SLAB, None, None), P(SLAB, None, None), P("y", SLAB), P(None, "y"))
    return jax.shard_map(
        local, mesh=split_mesh, in_specs=placed, out_specs=P("y", SLAB), check_vma=False
    )
```

```python
import functools

import jax
import jax.numpy as jnp
from jax import lax
from jax.experimental import pallas as pl
from jax.experimental.pallas import tpu as pltpu
from jax.sharding import Mesh
from jax.sharding import PartitionSpec as P

SLAB = ("z", "x", "c")
ALL = ("z", "x", "c", "y")
F32 = jnp.float32
BF16 = jnp.bfloat16
N = 512
H = 256
Q = 128
R = 64


def split(a):
    hi = a.astype(BF16)
    return hi, (a - hi.astype(F32)).astype(BF16)


def dot(a, b):
    return lax.dot_general(a, b, (((1,), (0,)), ((), ())), preferred_element_type=F32)


def mm(a, b):
    return dot(a[0], b[0]) + (dot(a[0], b[1]) + dot(a[1], b[0]))


def mm_small(a, b):
    ah, al = split(a)
    bh, bl = split(b)
    row = jnp.concatenate([bh, bl], axis=1)
    both = dot(jnp.concatenate([ah, al], axis=1), jnp.concatenate([row, row], axis=0))
    return both[:, :Q] + both[:, Q:]


def local_body(first_ref, diag_hbm, sub_hbm, right_hbm, bound_hbm, out_ref, diag_ref, sub_ref, right_ref, bound_ref, sems):
    loads = [
        pltpu.make_async_copy(src, dst, sems.at[i])
        for i, (src, dst) in enumerate([
            (diag_hbm, diag_ref), (sub_hbm, sub_ref), (right_hbm, right_ref), (bound_hbm, bound_ref)])
    ]
    for load in loads:
        load.start()
    loads[0].wait()
    row = lax.broadcasted_iota(jnp.int32, (Q, Q), 0)
    col = lax.broadcasted_iota(jnp.int32, (Q, Q), 1)
    eye = row == col

    def block(i, j):
        return diag_ref[0, j * Q:(j + 1) * Q, i * Q:(i + 1) * Q].T

    ups = [block(i, i) for i in range(4)]
    inv = []
    for u in ups:
        d = jnp.where(eye, u, 0.0)
        across = 1.0 / jnp.sum(d, axis=0, keepdims=True)
        down = 1.0 / jnp.sum(d, axis=1, keepdims=True)
        pair = ((row & 1) == 0) & (col == row + 1)
        inv.append(jnp.where(eye, across, jnp.where(pair, -(down * u) * across, 0.0)))
    for level in range(1, 7):
        rb, cb = row >> level, col >> level
        pick = ((rb & 1) == 0) & (cb == rb + 1)
        half = [mm_small(x, jnp.where(pick, u, 0.0)) for x, u in zip(inv, ups)]
        inv = [x - mm_small(h, x) for h, x in zip(half, inv)]
    tiles = []
    for i in (0, 2):
        off = mm_small(mm_small(inv[i], block(i, i + 1)), inv[i + 1])
        zero = jnp.zeros((Q, Q), F32)
        tiles.append(split(jnp.concatenate([
            jnp.concatenate([inv[i], -off], axis=1),
            jnp.concatenate([zero, inv[i + 1]], axis=1)], axis=0)))
    for load in loads[1:]:
        load.wait()
    left0 = jnp.concatenate([sub_ref[0, :H, :].T, right_ref[:, :H]], axis=0)
    right0 = jnp.concatenate([sub_ref[0, H:, :].T, right_ref[:, H:]], axis=0)
    left = mm(split(left0), tiles[0])
    cross = split(diag_ref[0, H:, :H].T)
    right = mm(split(right0 - mm(split(left), cross)), tiles[1])
    out_ref[:N, :H] = -left[:N]
    out_ref[:N, H:] = -right[:N]
    out_ref[N:, :H] = left[N:]
    out_ref[N:, H:] = right[N:]

    @pl.when(first_ref[0] == 1)
    def _():
        out_ref[N:, :] += mm(split(bound_ref[...]), split(out_ref[:N, :]))


def pair_body(core_ref, own_ref, other_ref, hi_ref, lo_ref, vec_ref):
    def go(first, second):
        both = mm(split(first[...]), split(second[:N, :]))
        hi, lo = split(both[:N])
        hi_ref[...] = hi
        lo_ref[...] = lo
        vec_ref[...] = both[N:] + second[N:, :]

    @pl.when(core_ref[0] == 0)
    def _():
        go(own_ref, other_ref)

    @pl.when(core_ref[0] == 1)
    def _():
        go(other_ref, own_ref)


def hop_body(got_ref, had_ref, hi_ref, lo_ref, vec_ref, in_ref, end_ref):
    total = had_ref[...] + got_ref[...]
    in_ref[...] = total
    end_ref[...] = vec_ref[...] + mm(split(total), (hi_ref[...], lo_ref[...]))


def last_body(core_ref, in_ref, end_ref, own_ref, out_ref):
    @pl.when(core_ref[0] == 0)
    def _():
        out_ref[...] = own_ref[N:, :] + mm(split(in_ref[...]), split(own_ref[:N, :]))

    @pl.when(core_ref[0] == 1)
    def _():
        out_ref[...] = end_ref[...]


def kernel(body, outs, name, scratch=()):
    smem = pl.BlockSpec(memory_space=pltpu.SMEM)
    vmem = pl.BlockSpec(memory_space=pltpu.VMEM)
    data = pl.BlockSpec(memory_space=pltpu.HBM) if scratch else vmem

    def call(*args):
        space = pltpu.HBM if scratch else pltpu.VMEM
        args = [a if a.dtype == jnp.int32 else pltpu.with_memory_space_constraint(a, space) for a in args]
        return pl.pallas_call(
            body,
            out_shape=jax.tree.map(lambda o: pltpu.VMEM(o.shape, o.dtype), outs),
            in_specs=[smem if a.dtype == jnp.int32 else data for a in args],
            out_specs=jax.tree.map(lambda _: vmem, outs),
            scratch_shapes=scratch,
            name=name,
            compiler_params=pltpu.CompilerParams(vmem_limit_bytes=16 << 20),
        )(*args)

    return call


def arr(rows, dtype=F32):
    return jax.ShapeDtypeStruct((rows, N), dtype)


def index(z, x, c, y):
    return ((z * 4 + x) * 2 + c) * 4 + y


def local(diag_blocks, sub_blocks, right_side, boundary):
    core = lax.axis_index("c").astype(jnp.int32).reshape(1)
    first = (lax.axis_index(SLAB) == 0).astype(jnp.int32).reshape(1)
    loads = [
        pltpu.VMEM((1, N, N), F32), pltpu.VMEM((1, N, N), F32), pltpu.VMEM((R, N), F32),
        pltpu.VMEM((R, N), F32), pltpu.SemaphoreType.DMA((4,)),
    ]
    own = kernel(local_body, arr(N + R), "local", loads)(
        first, diag_blocks, sub_blocks, right_side, boundary.T)
    other = lax.ppermute(own, "c", [(0, 1), (1, 0)])
    hi, lo, vec = kernel(pair_body, [arr(N, BF16), arr(N, BF16), arr(R)], "pair")(core, own, other)
    inflow = jnp.zeros((R, N), F32)
    end = vec
    hop = kernel(hop_body, [arr(R), arr(R)], "hop")
    for k in range(15):
        pairs = [(index(k // 4, k % 4, 1, y), index((k + 1) // 4, (k + 1) % 4, 1, y)) for y in range(4)]
        got = lax.ppermute(end, ALL, pairs)
        inflow, end = hop(got, inflow, hi, lo, vec)
    chips = [(z, x, y) for z in range(4) for x in range(4) for y in range(4)]
    down = lax.ppermute(inflow, ALL, [(index(z, x, 1, y), index(z, x, 0, y)) for z, x, y in chips])
    return kernel(last_body, arr(R), "last")(core, down, end, own)


def solution(mesh):
    shape = mesh.devices.reshape(4, 4, 2, 4)
    split_mesh = Mesh(shape, ALL)
    placed = (P(SLAB, None, None), P(SLAB, None, None), P("y", SLAB), P(None, "y"))
    return jax.shard_map(
        local, mesh=split_mesh, in_specs=placed, out_specs=P("y", SLAB), check_vma=False
    )
```

```python
import functools

import jax
import jax.numpy as jnp
from jax import lax
from jax.experimental import pallas as pl
from jax.experimental.pallas import tpu as pltpu
from jax.sharding import Mesh
from jax.sharding import PartitionSpec as P

SLAB = ("z", "x", "c")
ALL = ("z", "x", "c", "y")
F32 = jnp.float32
BF16 = jnp.bfloat16
N = 512
H = 256
Q = 128
R = 64


def split(a):
    hi = a.astype(BF16)
    return hi, (a - hi.astype(F32)).astype(BF16)


def dot(a, b):
    return lax.dot_general(a, b, (((1,), (0,)), ((), ())), preferred_element_type=F32)


def mm(a, b):
    return dot(a[0], b[0]) + (dot(a[0], b[1]) + dot(a[1], b[0]))


def mm_small(a, b):
    ah, al = split(a)
    bh, bl = split(b)
    row = jnp.concatenate([bh, bl], axis=1)
    both = dot(jnp.concatenate([ah, al], axis=1), jnp.concatenate([row, row], axis=0))
    return both[:, :Q] + both[:, Q:]


def local_body(me_ref, diag_hbm, sub_hbm, right_hbm, bound_hbm, out_ref, diag_ref, sub_ref, right_ref, bound_ref, sems):
    loads = [
        pltpu.make_async_copy(src, dst, sems.at[i])
        for i, (src, dst) in enumerate([
            (diag_hbm, diag_ref), (sub_hbm, sub_ref), (right_hbm, right_ref), (bound_hbm, bound_ref)])
    ]
    for load in loads:
        load.start()
    loads[0].wait()
    row = lax.broadcasted_iota(jnp.int32, (Q, Q), 0)
    col = lax.broadcasted_iota(jnp.int32, (Q, Q), 1)
    eye = row == col

    def block(i, j):
        return diag_ref[0, j * Q:(j + 1) * Q, i * Q:(i + 1) * Q].T

    ups = [block(i, i) for i in range(4)]
    inv = []
    for u in ups:
        d = jnp.where(eye, u, 0.0)
        across = 1.0 / jnp.sum(d, axis=0, keepdims=True)
        down = 1.0 / jnp.sum(d, axis=1, keepdims=True)
        pair = ((row & 1) == 0) & (col == row + 1)
        inv.append(jnp.where(eye, across, jnp.where(pair, -(down * u) * across, 0.0)))
    for level in range(1, 7):
        rb, cb = row >> level, col >> level
        pick = ((rb & 1) == 0) & (cb == rb + 1)
        half = [mm_small(x, jnp.where(pick, u, 0.0)) for x, u in zip(inv, ups)]
        inv = [x - mm_small(h, x) for h, x in zip(half, inv)]
    tiles = []
    for i in (0, 2):
        off = mm_small(mm_small(inv[i], block(i, i + 1)), inv[i + 1])
        zero = jnp.zeros((Q, Q), F32)
        tiles.append(split(jnp.concatenate([
            jnp.concatenate([inv[i], -off], axis=1),
            jnp.concatenate([zero, inv[i + 1]], axis=1)], axis=0)))
    for load in loads[1:]:
        load.wait()
    left0 = jnp.concatenate([sub_ref[0, :H, :].T, right_ref[:, :H]], axis=0)
    right0 = jnp.concatenate([sub_ref[0, H:, :].T, right_ref[:, H:]], axis=0)
    left = mm(split(left0), tiles[0])
    cross = split(diag_ref[0, H:, :H].T)
    right = mm(split(right0 - mm(split(left), cross)), tiles[1])
    out_ref[:N, :H] = -left[:N]
    out_ref[:N, H:] = -right[:N]
    out_ref[N:, :H] = left[N:]
    out_ref[N:, H:] = right[N:]

    @pl.when(me_ref[0] < 4)
    def _():
        out_ref[N:, :] += mm(split(bound_ref[...]), split(out_ref[:N, :]))


def core_of(me_ref):
    return (me_ref[0] >> 2) & 1


def pair_body(me_ref, own_ref, other_ref, full_ref, hi_ref, lo_ref, vec_ref):
    def go(first, second):
        both = mm(split(first[...]), split(second[:N, :]))
        vec = both[N:] + second[N:, :]
        hi_ref[...], lo_ref[...] = split(both[:N])
        full_ref[:N, :] = both[:N]
        full_ref[N:, :] = vec
        vec_ref[...] = vec

    @pl.when(core_of(me_ref) == 0)
    def _():
        go(own_ref, other_ref)

    @pl.when(core_of(me_ref) == 1)
    def _():
        go(other_ref, own_ref)


def hop_body(got_ref, had_ref, hi_ref, lo_ref, vec_ref, in_ref, end_ref):
    total = had_ref[...] + got_ref[...]
    in_ref[...] = total
    end_ref[...] = vec_ref[...] + mm(split(total), (hi_ref[...], lo_ref[...]))


def join_body(me_ref, before_ref, hi_ref, lo_ref, vec_ref, end_ref, jhi_ref, jlo_ref, jvec_ref):
    both = mm(split(before_ref[...]), (hi_ref[...], lo_ref[...]))
    jhi_ref[...], jlo_ref[...] = split(both[:N])
    jvec_ref[...] = jnp.where(me_ref[0] < 32, end_ref[...], both[N:] + vec_ref[...])


def tail_body(me_ref, walked_ref, got_ref, in_ref, before_ref, hi_ref, lo_ref, vec_ref, end_ref, out_ref, last_ref):
    line = me_ref[0] >> 5
    odd = (me_ref[0] >> 3) & 1

    @pl.when(line == 0)
    def _():
        out_ref[...] = walked_ref[...]
        last_ref[...] = end_ref[...]

    @pl.when((line > 0) & (odd == 1))
    def _():
        out_ref[...] = before_ref[N:, :] + mm(split(in_ref[...]), split(before_ref[:N, :]))
        last_ref[...] = end_ref[...]

    @pl.when((line > 0) & (odd == 0))
    def _():
        out_ref[...] = got_ref[...]
        last_ref[...] = vec_ref[...] + mm(split(got_ref[...]), (hi_ref[...], lo_ref[...]))


def last_body(me_ref, in_ref, end_ref, own_ref, out_ref):
    @pl.when(core_of(me_ref) == 0)
    def _():
        out_ref[...] = own_ref[N:, :] + mm(split(in_ref[...]), split(own_ref[:N, :]))

    @pl.when(core_of(me_ref) == 1)
    def _():
        out_ref[...] = end_ref[...]


def kernel(body, outs, name, scratch=()):
    smem = pl.BlockSpec(memory_space=pltpu.SMEM)
    space = pltpu.HBM if scratch else pltpu.VMEM
    data = pl.BlockSpec(memory_space=space)

    def call(*args):
        args = [a if a.dtype == jnp.int32 else pltpu.with_memory_space_constraint(a, space) for a in args]
        return pl.pallas_call(
            body,
            out_shape=outs,
            in_specs=[smem if a.dtype == jnp.int32 else data for a in args],
            out_specs=jax.tree.map(lambda _: pl.BlockSpec(memory_space=pltpu.VMEM), outs),
            scratch_shapes=scratch,
            name=name,
            compiler_params=pltpu.CompilerParams(vmem_limit_bytes=16 << 20),
        )(*args)

    return call


def arr(rows, dtype=F32):
    return pltpu.VMEM((rows, N), dtype)


def links(chips):
    return [(chip_a * 8 + 4 + y, chip_b * 8 + 4 + y) for chip_a, chip_b in chips for y in range(4)]


def local(diag_blocks, sub_blocks, right_side, boundary):
    me = lax.axis_index(ALL).astype(jnp.int32).reshape(1)
    loads = [
        pltpu.VMEM((1, N, N), F32), pltpu.VMEM((1, N, N), F32), pltpu.VMEM((R, N), F32),
        pltpu.VMEM((R, N), F32), pltpu.SemaphoreType.DMA((4,)),
    ]
    own = kernel(local_body, arr(N + R), "local", loads)(
        me, diag_blocks, sub_blocks, right_side, boundary.T)
    other = lax.ppermute(own, "c", [(0, 1), (1, 0)])
    full, hi, lo, vec = kernel(
        pair_body, [arr(N + R), arr(N, BF16), arr(N, BF16), arr(R)], "pair")(me, own, other)
    before = lax.ppermute(full, ALL, links([(k, k + 1) for k in range(4, 16, 2)]))
    hop = kernel(hop_body, [arr(R), arr(R)], "hop")
    walked, end = jnp.zeros((R, N), F32), vec
    for k in range(3):
        walked, end = hop(lax.ppermute(end, ALL, links([(k, k + 1)])), walked, hi, lo, vec)
    step = lax.ppermute(end, ALL, links([(3, 5)]))
    jhi, jlo, jvec = kernel(join_body, [arr(N, BF16), arr(N, BF16), arr(R)], "join")(
        me, before, hi, lo, vec, end)
    inflow, end = hop(step, jnp.zeros((R, N), F32), jhi, jlo, jvec)
    for k in range(5, 15, 2):
        inflow, end = hop(lax.ppermute(end, ALL, links([(k, k + 2)])), inflow, jhi, jlo, jvec)
    got = lax.ppermute(end, ALL, links([(k, k + 1) for k in range(3, 15, 2)]))
    inflow, end = kernel(tail_body, [arr(R), arr(R)], "tail")(
        me, walked, got, inflow, before, hi, lo, vec, end)
    down = lax.ppermute(inflow, "c", [(0, 1), (1, 0)])
    return kernel(last_body, jax.ShapeDtypeStruct((R, N), F32), "last")(me, down, end, own)


def solution(mesh):
    shape = mesh.devices.reshape(4, 4, 2, 4)
    split_mesh = Mesh(shape, ALL)
    placed = (P(SLAB, None, None), P(SLAB, None, None), P("y", SLAB), P(None, "y"))
    return jax.shard_map(
        local, mesh=split_mesh, in_specs=placed, out_specs=P("y", SLAB), check_vma=False
    )
```

```python
import functools

import jax
import jax.numpy as jnp
from jax import lax
from jax.experimental import pallas as pl
from jax.experimental.pallas import tpu as pltpu
from jax.sharding import Mesh
from jax.sharding import PartitionSpec as P


SLAB = ("z", "x", "c")
ALL = ("z", "x", "c", "y")
F32 = jnp.float32
BF16 = jnp.bfloat16
N = 512
H = 256
Q = 128
R = 64


def split(a):
    hi = a.astype(BF16)
    return hi, (a - hi.astype(F32)).astype(BF16)


def dot(a, b):
    return lax.dot_general(a, b, (((1,), (0,)), ((), ())), preferred_element_type=F32)


def mm(a, b):
    return dot(a[0], b[0]) + (dot(a[0], b[1]) + dot(a[1], b[0]))


def mm_small(a, b):
    ah, al = split(a)
    bh, bl = split(b)
    row = jnp.concatenate([bh, bl], axis=1)
    both = dot(jnp.concatenate([ah, al], axis=1), jnp.concatenate([row, row], axis=0))
    return both[:, :Q] + both[:, Q:]


def local_body(me_ref, diag_hbm, sub_hbm, right_hbm, bound_hbm, out_ref, diag_ref, sub_ref, right_ref, bound_ref, sems):
    loads = [
        pltpu.make_async_copy(src, dst, sems.at[i])
        for i, (src, dst) in enumerate([
            (diag_hbm, diag_ref), (sub_hbm, sub_ref), (right_hbm, right_ref), (bound_hbm, bound_ref)])
    ]
    for load in loads:
        load.start()
    loads[0].wait()
    row = lax.broadcasted_iota(jnp.int32, (Q, Q), 0)
    col = lax.broadcasted_iota(jnp.int32, (Q, Q), 1)
    eye = row == col

    def block(i, j):
        return diag_ref[0, j * Q:(j + 1) * Q, i * Q:(i + 1) * Q].T

    ups = [block(i, i) for i in range(4)]
    inv = []
    for u in ups:
        d = jnp.where(eye, u, 0.0)
        across = 1.0 / jnp.sum(d, axis=0, keepdims=True)
        down = 1.0 / jnp.sum(d, axis=1, keepdims=True)
        pair = ((row & 1) == 0) & (col == row + 1)
        inv.append(jnp.where(eye, across, jnp.where(pair, -(down * u) * across, 0.0)))
    for level in range(1, 7):
        rb, cb = row >> level, col >> level
        pick = ((rb & 1) == 0) & (cb == rb + 1)
        half = [mm_small(x, jnp.where(pick, u, 0.0)) for x, u in zip(inv, ups)]
        inv = [x - mm_small(h, x) for h, x in zip(half, inv)]
    tiles = []
    for i in (0, 2):
        off = mm_small(mm_small(inv[i], block(i, i + 1)), inv[i + 1])
        zero = jnp.zeros((Q, Q), F32)
        tiles.append(split(jnp.concatenate([
            jnp.concatenate([inv[i], -off], axis=1),
            jnp.concatenate([zero, inv[i + 1]], axis=1)], axis=0)))
    for load in loads[1:]:
        load.wait()
    left0 = jnp.concatenate([sub_ref[0, :H, :].T, right_ref[:, :H]], axis=0)
    right0 = jnp.concatenate([sub_ref[0, H:, :].T, right_ref[:, H:]], axis=0)
    left = mm(split(left0), tiles[0])
    cross = split(diag_ref[0, H:, :H].T)
    right = mm(split(right0 - mm(split(left), cross)), tiles[1])
    out_ref[:N, :H] = -left[:N]
    out_ref[:N, H:] = -right[:N]
    out_ref[N:, :H] = left[N:]
    out_ref[N:, H:] = right[N:]

    @pl.when(me_ref[0] < 4)
    def _():
        out_ref[N:, :] += mm(split(bound_ref[...]), split(out_ref[:N, :]))


def core_of(me_ref):
    return (me_ref[0] >> 2) & 1


def pair_body(me_ref, own_ref, other_ref, full_ref, piece_ref, hi_ref, lo_ref, vec_ref):
    def go(first, second):
        both = mm(split(first[...]), split(second[:N, :]))
        vec = both[N:] + second[N:, :]
        hi_ref[...], lo_ref[...] = split(both[:N])
        full_ref[:N, :] = both[:N]
        full_ref[N:, :] = vec
        vec_ref[...] = vec

    @pl.when(core_of(me_ref) == 0)
    def _():
        go(own_ref, other_ref)

    @pl.when(core_of(me_ref) == 1)
    def _():
        go(other_ref, own_ref)

    piece_ref[:Q, :] = full_ref[pl.ds((me_ref[0] & 3) * Q, Q), :]
    piece_ref[Q:, :] = vec_ref[...]


def arrived(me_ref, value, news):
    for ref, chips in news:
        here = functools.reduce(jnp.logical_or, [(me_ref[0] >> 3) == chip for chip in chips])
        value = jnp.where(here, ref[...], value)
    return value


def hop_body(chip, me_ref, got_ref, had_ref, hi_ref, lo_ref, vec_ref, in_ref, end_ref):
    total = arrived(me_ref, had_ref[...], [(got_ref, [chip])])
    in_ref[...] = total
    end_ref[...] = vec_ref[...] + mm(split(total), (hi_ref[...], lo_ref[...]))


def pick_body(chips, me_ref, *refs):
    *news, out_ref = refs
    out_ref[...] = arrived(me_ref, jnp.zeros((R, N), F32), list(zip(news, chips)))


def near_body(full_ref, hi_ref, lo_ref, vec_ref):
    hi_ref[...], lo_ref[...] = split(full_ref[:N, :])
    vec_ref[...] = full_ref[N:, :]


def far_body(me_ref, *refs):
    quarter_ref, *pieces, hi_ref, lo_ref, vec_ref = refs
    for s, piece in zip((0, 1, 3, 2), [quarter_ref, *pieces]):
        rows = pl.ds(((me_ref[0] + s) & 3) * Q, Q)
        hi_ref[rows, :], lo_ref[rows, :] = split(piece[:Q, :])
    vec_ref[...] = quarter_ref[Q:, :]


def line_body(chips, me_ref, *refs):
    maps, had_ref, news, (in_ref, end_ref) = refs[:12], refs[12], refs[13:-2], refs[-2:]
    inflow = arrived(me_ref, had_ref[...], list(zip(news, chips)))
    in_ref[...] = inflow
    for x in range(4):
        @pl.when(((me_ref[0] >> 3) & 3) == x)
        def _():
            current = inflow
            for chip in range(4):
                hi, lo, vec = maps[3 * ((chip - x) % 4):][:3]
                current = vec[...] + mm(split(current), (hi[...], lo[...]))
            end_ref[...] = current


def final_body(chips, me_ref, *refs):
    maps, (walked_ref, walk_end_ref, had_ref) = refs[:12], refs[12:15]
    news, (in_ref, end_ref) = refs[15:-2], refs[-2:]
    line = me_ref[0] >> 5

    @pl.when(line == 0)
    def _():
        in_ref[...] = walked_ref[...]
        end_ref[...] = walk_end_ref[...]

    for x in range(4):
        @pl.when((line > 0) & (((me_ref[0] >> 3) & 3) == x))
        def _():
            current = arrived(me_ref, had_ref[...], list(zip(news, chips)))
            for chip in range(x + 1):
                if chip == x:
                    in_ref[...] = current
                hi, lo, vec = maps[3 * ((chip - x) % 4):][:3]
                current = vec[...] + mm(split(current), (hi[...], lo[...]))
            end_ref[...] = current


def last_body(me_ref, in_ref, end_ref, own_ref, out_ref):
    @pl.when(core_of(me_ref) == 0)
    def _():
        out_ref[...] = own_ref[N:, :] + mm(split(in_ref[...]), split(own_ref[:N, :]))

    @pl.when(core_of(me_ref) == 1)
    def _():
        out_ref[...] = end_ref[...]


def kernel(body, outs, scratch=(), space=pltpu.VMEM):
    smem = pl.BlockSpec(memory_space=pltpu.SMEM)
    data = pl.BlockSpec(memory_space=space)

    def call(*args):
        args = [a if a.dtype == jnp.int32 else pltpu.with_memory_space_constraint(a, space) for a in args]
        return pl.pallas_call(
            body,
            out_shape=outs,
            in_specs=[smem if a.dtype == jnp.int32 else data for a in args],
            out_specs=jax.tree.map(lambda _: pl.BlockSpec(memory_space=pltpu.VMEM), outs),
            scratch_shapes=scratch,
            compiler_params=pltpu.CompilerParams(vmem_limit_bytes=16 << 20),
        )(*args)

    return call


def arr(rows, dtype=F32):
    return pltpu.VMEM((rows, N), dtype)


def device(z, x, core, y):
    return ((z * 4 + x) * 2 + core) * 4 + y


def complete(moves):
    pairs = dict(moves)
    taken = set(pairs.values())
    for source, target in list(pairs.items()):
        for a, b in ((target, target ^ 4), (target ^ 4, source ^ 4), (source ^ 4, source)):
            if a not in pairs and b not in taken:
                pairs[a] = b
                taken.add(b)
    for i in range(128):
        if i not in pairs:
            pairs[i] = i ^ 4
            taken.add(i ^ 4)
    assert len(taken) == 128 and all(a != b for a, b in pairs.items())
    return sorted(pairs.items())


def hops(pairs):
    return complete([(device(*a, 1, y), device(*b, 1, y)) for a, b in pairs for y in range(4)])


LINES = [(z, x, y) for z in range(1, 4) for x in range(4) for y in range(4)]


def ring(x_step, y_step):
    return [(device(z, (x + x_step) % 4, 1, (y + y_step) % 4), device(z, x, 1, y)) for z, x, y in LINES]


def full_ring(x_step, y_step):
    return complete(ring(x_step, y_step) + [(device(z, x, 0, y), device(z % 3 + 1, x, 0, y)) for z, x, y in LINES])


def local(diag_blocks, sub_blocks, right_side, boundary):
    def send(value, pairs):
        return lax.ppermute(value, ALL, pairs)

    me = lax.axis_index(ALL).astype(jnp.int32).reshape(1)
    loads = [
        pltpu.VMEM((1, N, N), F32), pltpu.VMEM((1, N, N), F32), pltpu.VMEM((R, N), F32),
        pltpu.VMEM((R, N), F32), pltpu.SemaphoreType.DMA((4,)),
    ]
    own = kernel(local_body, arr(N + R), loads, pltpu.HBM)(
        me, diag_blocks, sub_blocks, right_side, boundary.T)
    other = lax.ppermute(own, "c", [(0, 1), (1, 0)])
    weights, two = [arr(N, BF16), arr(N, BF16), arr(R)], [arr(R), arr(R)]
    full, piece, *here = kernel(pair_body, [arr(N + R), arr(Q + R)] + weights)(me, own, other)
    hi, lo, vec = here

    quarters = [send(piece, full_ring(2, 0))]
    left = send(full, ring(-1, 0))
    right = send(full, ring(1, 0))
    quarters += [send(quarters[0][:Q], full_ring(0, s)) for s in (1, 3, 2)]

    walked, walk_end = jnp.zeros((R, N), F32), vec
    for x in range(3):
        got = send(walk_end, hops([((0, x), (0, x + 1))]))
        hop = kernel(functools.partial(hop_body, x + 1), two)
        walked, walk_end = hop(me, got, walked, hi, lo, vec)
    first = send(walk_end, hops([((0, 3), (1, 3))]))
    second = send(walk_end, hops([((0, 3), (1, 0))]))
    inflow = kernel(functools.partial(pick_body, [(7,), (4,)]), arr(R))(me, first, second)
    third = send(inflow, hops([((1, 3), (1, 2)), ((1, 0), (1, 1))]))

    far = kernel(far_body, weights)(me, *quarters)
    near = kernel(near_body, weights)
    maps = [*here, *near(right), *far, *near(left)]

    line = kernel(functools.partial(line_body, [(5, 6)]), two)
    inflow, end = line(me, *maps, inflow, third)
    fourth = send(end, hops([((1, x), (2, x)) for x in range(4)]))
    line = kernel(functools.partial(line_body, [(8, 9, 10, 11)]), two)
    inflow, end = line(me, *maps, inflow, fourth)
    fifth = send(end, hops([((2, x), (3, x)) for x in range(4)]))
    inflow, end = kernel(functools.partial(final_body, [(12, 13, 14, 15)]), two)(
        me, *maps, walked, walk_end, inflow, fifth)
    down = lax.ppermute(inflow, "c", [(0, 1), (1, 0)])
    return kernel(last_body, jax.ShapeDtypeStruct((R, N), F32))(me, down, end, own)


def solution(mesh):
    split_mesh = Mesh(mesh.devices.reshape(4, 4, 2, 4), ALL)
    placed = (P(SLAB, None, None), P(SLAB, None, None), P("y", SLAB), P(None, "y"))

    return jax.shard_map(local, mesh=split_mesh, in_specs=placed, out_specs=P("y", SLAB), check_vma=False)
```

```python
import functools

import jax
import jax.numpy as jnp
from jax import lax
from jax.experimental import pallas as pl
from jax.experimental.pallas import tpu as pltpu
from jax.sharding import Mesh
from jax.sharding import PartitionSpec as P


SLAB = ("z", "x", "c")
ALL = ("z", "x", "c", "y")
F32 = jnp.float32
BF16 = jnp.bfloat16
N = 512
H = 256
Q = 128
R = 64


def split(a):
    hi = a.astype(BF16)
    return hi, (a - hi.astype(F32)).astype(BF16)


def dot(a, b):
    return lax.dot_general(a, b, (((1,), (0,)), ((), ())), preferred_element_type=F32)


def mm(a, b):
    return dot(a[0], b[0]) + (dot(a[0], b[1]) + dot(a[1], b[0]))


def mm_small(a, b):
    ah, al = split(a)
    bh, bl = split(b)
    row = jnp.concatenate([bh, bl], axis=1)
    both = dot(jnp.concatenate([ah, al], axis=1), jnp.concatenate([row, row], axis=0))
    return both[:, :Q] + both[:, Q:]


def local_body(me_ref, diag_hbm, sub_hbm, right_hbm, bound_hbm, out_ref, diag_ref, sub_ref, right_ref, bound_ref, sems):
    loads = [
        pltpu.make_async_copy(src, dst, sems.at[i])
        for i, (src, dst) in enumerate([
            (diag_hbm, diag_ref), (sub_hbm, sub_ref), (right_hbm, right_ref), (bound_hbm, bound_ref)])
    ]
    for load in loads:
        load.start()
    loads[0].wait()
    row = lax.broadcasted_iota(jnp.int32, (Q, Q), 0)
    col = lax.broadcasted_iota(jnp.int32, (Q, Q), 1)
    eye = row == col

    def block(i, j):
        return diag_ref[0, j * Q:(j + 1) * Q, i * Q:(i + 1) * Q].T

    ups = [block(i, i) for i in range(4)]
    inv = []
    for u in ups:
        d = jnp.where(eye, u, 0.0)
        across = 1.0 / jnp.sum(d, axis=0, keepdims=True)
        down = 1.0 / jnp.sum(d, axis=1, keepdims=True)
        pair = ((row & 1) == 0) & (col == row + 1)
        inv.append(jnp.where(eye, across, jnp.where(pair, -(down * u) * across, 0.0)))
    for level in range(1, 7):
        rb, cb = row >> level, col >> level
        pick = ((rb & 1) == 0) & (cb == rb + 1)
        half = [mm_small(x, jnp.where(pick, u, 0.0)) for x, u in zip(inv, ups)]
        inv = [x - mm_small(h, x) for h, x in zip(half, inv)]
    tiles = []
    for i in (0, 2):
        off = mm_small(mm_small(inv[i], block(i, i + 1)), inv[i + 1])
        zero = jnp.zeros((Q, Q), F32)
        tiles.append(split(jnp.concatenate([
            jnp.concatenate([inv[i], -off], axis=1),
            jnp.concatenate([zero, inv[i + 1]], axis=1)], axis=0)))
    for load in loads[1:]:
        load.wait()
    left0 = jnp.concatenate([sub_ref[0, :H, :].T, right_ref[:, :H]], axis=0)
    right0 = jnp.concatenate([sub_ref[0, H:, :].T, right_ref[:, H:]], axis=0)
    left = mm(split(left0), tiles[0])
    cross = split(diag_ref[0, H:, :H].T)
    right = mm(split(right0 - mm(split(left), cross)), tiles[1])
    out_ref[:N, :H] = -left[:N]
    out_ref[:N, H:] = -right[:N]
    out_ref[N:, :H] = left[N:]
    out_ref[N:, H:] = right[N:]

    @pl.when(me_ref[0] < 4)
    def _():
        out_ref[N:, :] += mm(split(bound_ref[...]), split(out_ref[:N, :]))


def core_of(me_ref):
    return (me_ref[0] >> 2) & 1


def pair_body(me_ref, own_ref, other_ref, full_ref, piece_ref, hi_ref, lo_ref, vec_ref):
    def go(first, second):
        both = mm(split(first[...]), split(second[:N, :]))
        vec = both[N:] + second[N:, :]
        hi_ref[...], lo_ref[...] = split(both[:N])
        full_ref[:N, :] = both[:N]
        full_ref[N:, :] = vec
        vec_ref[...] = vec

    @pl.when(core_of(me_ref) == 0)
    def _():
        go(own_ref, other_ref)

    @pl.when(core_of(me_ref) == 1)
    def _():
        go(other_ref, own_ref)

    piece_ref[:Q, :] = full_ref[pl.ds((me_ref[0] & 3) * Q, Q), :]
    piece_ref[Q:, :] = vec_ref[...]


def arrived(me_ref, value, news):
    for ref, chips in news:
        here = functools.reduce(jnp.logical_or, [(me_ref[0] >> 3) == chip for chip in chips])
        value = jnp.where(here, ref[...], value)
    return value


def hop_body(chip, me_ref, got_ref, had_ref, old_ref, hi_ref, lo_ref, vec_ref, in_ref, end_ref):
    here = (me_ref[0] >> 2) == 2 * chip + 1

    @pl.when(here)
    def _():
        in_ref[...] = got_ref[...]
        end_ref[...] = vec_ref[...] + mm(split(got_ref[...]), (hi_ref[...], lo_ref[...]))

    @pl.when(jnp.logical_not(here))
    def _():
        in_ref[...] = had_ref[...]
        end_ref[...] = old_ref[...]


def upper_only(me_ref):
    return (core_of(me_ref) == 1) & (me_ref[0] >= 32)


def pick_body(chips, me_ref, *refs):
    *news, out_ref = refs
    out_ref[...] = arrived(me_ref, jnp.zeros((R, N), F32), list(zip(news, chips)))


def near_body(me_ref, full_ref, hi_ref, lo_ref, vec_ref):
    @pl.when(upper_only(me_ref))
    def _():
        hi_ref[...], lo_ref[...] = split(full_ref[:N, :])
        vec_ref[...] = full_ref[N:, :]


def far_body(me_ref, *refs):
    quarter_ref, *pieces, hi_ref, lo_ref, vec_ref = refs

    @pl.when(upper_only(me_ref))
    def _():
        for s, piece in zip((0, 1, 3, 2), [quarter_ref, *pieces]):
            rows = pl.ds(((me_ref[0] + s) & 3) * Q, Q)
            hi_ref[rows, :], lo_ref[rows, :] = split(piece[:Q, :])
        vec_ref[...] = quarter_ref[Q:, :]


def line_body(which, chips, me_ref, *refs):
    maps, had_ref, news, (in_ref, end_ref) = refs[:12], refs[12], refs[13:-2], refs[-2:]
    inflow = arrived(me_ref, had_ref[...], list(zip(news, chips)))
    in_ref[...] = inflow
    for x in range(4):
        @pl.when((me_ref[0] >> 2) == 8 * which + 2 * x + 1)
        def _():
            current = inflow
            for chip in range(4):
                hi, lo, vec = maps[3 * ((chip - x) % 4):][:3]
                current = vec[...] + mm(split(current), (hi[...], lo[...]))
            end_ref[...] = current


def final_body(chips, me_ref, *refs):
    maps, (walked_ref, walk_end_ref, had_ref) = refs[:12], refs[12:15]
    news, (in_ref, end_ref) = refs[15:-2], refs[-2:]
    line = me_ref[0] >> 5

    @pl.when(line == 0)
    def _():
        in_ref[...] = walked_ref[...]
        end_ref[...] = walk_end_ref[...]

    for x in range(4):
        @pl.when(upper_only(me_ref) & (((me_ref[0] >> 3) & 3) == x))
        def _():
            current = arrived(me_ref, had_ref[...], list(zip(news, chips)))
            for chip in range(x + 1):
                if chip == x:
                    in_ref[...] = current
                hi, lo, vec = maps[3 * ((chip - x) % 4):][:3]
                current = vec[...] + mm(split(current), (hi[...], lo[...]))
            end_ref[...] = current


def last_body(me_ref, in_ref, end_ref, own_ref, out_ref):
    @pl.when(core_of(me_ref) == 0)
    def _():
        out_ref[...] = own_ref[N:, :] + mm(split(in_ref[...]), split(own_ref[:N, :]))

    @pl.when(core_of(me_ref) == 1)
    def _():
        out_ref[...] = end_ref[...]


def kernel(body, outs, scratch=(), space=pltpu.VMEM):
    smem = pl.BlockSpec(memory_space=pltpu.SMEM)
    data = pl.BlockSpec(memory_space=space)

    def call(*args):
        args = [a if a.dtype == jnp.int32 else pltpu.with_memory_space_constraint(a, space) for a in args]
        return pl.pallas_call(
            body,
            out_shape=outs,
            in_specs=[smem if a.dtype == jnp.int32 else data for a in args],
            out_specs=jax.tree.map(lambda _: pl.BlockSpec(memory_space=pltpu.VMEM), outs),
            scratch_shapes=scratch,
            compiler_params=pltpu.CompilerParams(vmem_limit_bytes=16 << 20),
        )(*args)

    return call


def arr(rows, dtype=F32):
    return pltpu.VMEM((rows, N), dtype)


def device(z, x, core, y):
    return ((z * 4 + x) * 2 + core) * 4 + y


def complete(moves):
    pairs = dict(moves)
    taken = set(pairs.values())
    for source, target in list(pairs.items()):
        for a, b in ((target, target ^ 4), (target ^ 4, source ^ 4), (source ^ 4, source)):
            if a not in pairs and b not in taken:
                pairs[a] = b
                taken.add(b)
    for i in range(128):
        if i not in pairs:
            pairs[i] = i ^ 4
            taken.add(i ^ 4)
    assert len(taken) == 128 and all(a != b for a, b in pairs.items())
    return sorted(pairs.items())


def hops(pairs):
    return complete([(device(*a, 1, y), device(*b, 1, y)) for a, b in pairs for y in range(4)])


LINES = [(z, x, y) for z in range(1, 4) for x in range(4) for y in range(4)]


def ring(x_step, y_step):
    return [(device(z, (x + x_step) % 4, 1, (y + y_step) % 4), device(z, x, 1, y)) for z, x, y in LINES]


def full_ring(x_step, y_step):
    return complete(ring(x_step, y_step) + [(device(z, x, 0, y), device(z % 3 + 1, x, 0, y)) for z, x, y in LINES])


def local(diag_blocks, sub_blocks, right_side, boundary):
    def send(value, pairs):
        return lax.ppermute(value, ALL, pairs)

    me = lax.axis_index(ALL).astype(jnp.int32).reshape(1)
    loads = [
        pltpu.VMEM((1, N, N), F32), pltpu.VMEM((1, N, N), F32), pltpu.VMEM((R, N), F32),
        pltpu.VMEM((R, N), F32), pltpu.SemaphoreType.DMA((4,)),
    ]
    own = kernel(local_body, arr(N + R), loads, pltpu.HBM)(
        me, diag_blocks, sub_blocks, right_side, boundary.T)
    other = lax.ppermute(own, "c", [(0, 1), (1, 0)])
    weights, two = [arr(N, BF16), arr(N, BF16), arr(R)], [arr(R), arr(R)]
    full, piece, *here = kernel(pair_body, [arr(N + R), arr(Q + R)] + weights)(me, own, other)
    hi, lo, vec = here

    quarters = [send(piece, full_ring(2, 0))]
    left = send(full, ring(-1, 0))
    right = send(full, ring(1, 0))
    quarters += [send(quarters[0][:Q], full_ring(0, s)) for s in (1, 3, 2)]

    walked, walk_end = jnp.zeros((R, N), F32), vec
    for x in range(3):
        got = send(walk_end, hops([((0, x), (0, x + 1))]))
        hop = kernel(functools.partial(hop_body, x + 1), two)
        walked, walk_end = hop(me, got, walked, walk_end, hi, lo, vec)
    first = send(walk_end, hops([((0, 3), (1, 3))]))
    second = send(walk_end, hops([((0, 3), (1, 0))]))
    inflow = kernel(functools.partial(pick_body, [(7,), (4,)]), arr(R))(me, first, second)
    third = send(inflow, hops([((1, 3), (1, 2)), ((1, 0), (1, 1))]))

    far = kernel(far_body, weights)(me, *quarters)
    near = kernel(near_body, weights)
    maps = [*here, *near(me, right), *far, *near(me, left)]

    line = kernel(functools.partial(line_body, 1, [(5, 6)]), two)
    inflow, end = line(me, *maps, inflow, third)
    fourth = send(end, hops([((1, x), (2, x)) for x in range(4)]))
    line = kernel(functools.partial(line_body, 2, [(8, 9, 10, 11)]), two)
    inflow, end = line(me, *maps, inflow, fourth)
    fifth = send(end, hops([((2, x), (3, x)) for x in range(4)]))
    inflow, end = kernel(functools.partial(final_body, [(12, 13, 14, 15)]), two)(
        me, *maps, walked, walk_end, inflow, fifth)
    down = lax.ppermute(inflow, "c", [(0, 1), (1, 0)])
    return kernel(last_body, jax.ShapeDtypeStruct((R, N), F32))(me, down, end, own)


def solution(mesh):
    split_mesh = Mesh(mesh.devices.reshape(4, 4, 2, 4), ALL)
    placed = (P(SLAB, None, None), P(SLAB, None, None), P("y", SLAB), P(None, "y"))

    return jax.shard_map(local, mesh=split_mesh, in_specs=placed, out_specs=P("y", SLAB), check_vma=False)
```

```python
import functools

import jax
import jax.numpy as jnp
from jax import lax
from jax.experimental import pallas as pl
from jax.experimental.pallas import tpu as pltpu
from jax.sharding import Mesh
from jax.sharding import PartitionSpec as P


SLAB = ("z", "x", "c")
ALL = ("z", "x", "c", "y")
F32 = jnp.float32
BF16 = jnp.bfloat16
N = 512
H = 256
Q = 128
R = 64


def split(a):
    hi = a.astype(BF16)
    return hi, (a - hi.astype(F32)).astype(BF16)


def dot(a, b):
    return lax.dot_general(a, b, (((1,), (0,)), ((), ())), preferred_element_type=F32)


def mm(a, b):
    return dot(a[0], b[0]) + (dot(a[0], b[1]) + dot(a[1], b[0]))


def mm_small(a, b):
    ah, al = split(a)
    bh, bl = split(b)
    row = jnp.concatenate([bh, bl], axis=1)
    both = dot(jnp.concatenate([ah, al], axis=1), jnp.concatenate([row, row], axis=0))
    return both[:, :Q] + both[:, Q:]


def local_body(me_ref, diag_hbm, sub_hbm, right_hbm, bound_hbm, out_ref, diag_ref, sub_ref, right_ref, bound_ref, sems):
    loads = [
        pltpu.make_async_copy(src, dst, sems.at[i])
        for i, (src, dst) in enumerate([
            (diag_hbm, diag_ref), (sub_hbm, sub_ref), (right_hbm, right_ref), (bound_hbm, bound_ref)])
    ]
    for load in loads:
        load.start()
    loads[0].wait()
    row = lax.broadcasted_iota(jnp.int32, (Q, Q), 0)
    col = lax.broadcasted_iota(jnp.int32, (Q, Q), 1)
    eye = row == col

    def block(i, j):
        return diag_ref[0, j * Q:(j + 1) * Q, i * Q:(i + 1) * Q].T

    ups = [block(i, i) for i in range(4)]
    inv = []
    for u in ups:
        d = jnp.where(eye, u, 0.0)
        across = 1.0 / jnp.sum(d, axis=0, keepdims=True)
        down = 1.0 / jnp.sum(d, axis=1, keepdims=True)
        pair = ((row & 1) == 0) & (col == row + 1)
        inv.append(jnp.where(eye, across, jnp.where(pair, -(down * u) * across, 0.0)))
    for level in range(1, 7):
        rb, cb = row >> level, col >> level
        pick = ((rb & 1) == 0) & (cb == rb + 1)
        half = [mm_small(x, jnp.where(pick, u, 0.0)) for x, u in zip(inv, ups)]
        inv = [x - mm_small(h, x) for h, x in zip(half, inv)]
    tiles = []
    for i in (0, 2):
        off = mm_small(mm_small(inv[i], block(i, i + 1)), inv[i + 1])
        zero = jnp.zeros((Q, Q), F32)
        tiles.append(split(jnp.concatenate([
            jnp.concatenate([inv[i], -off], axis=1),
            jnp.concatenate([zero, inv[i + 1]], axis=1)], axis=0)))
    for load in loads[1:]:
        load.wait()
    left0 = jnp.concatenate([sub_ref[0, :H, :].T, right_ref[:, :H]], axis=0)
    right0 = jnp.concatenate([sub_ref[0, H:, :].T, right_ref[:, H:]], axis=0)
    left = mm(split(left0), tiles[0])
    cross = split(diag_ref[0, H:, :H].T)
    right = mm(split(right0 - mm(split(left), cross)), tiles[1])
    out_ref[:N, :H] = -left[:N]
    out_ref[:N, H:] = -right[:N]
    out_ref[N:, :H] = left[N:]
    out_ref[N:, H:] = right[N:]

    @pl.when(me_ref[0] < 4)
    def _():
        out_ref[N:, :] += mm(split(bound_ref[...]), split(out_ref[:N, :]))


def core_of(me_ref):
    return (me_ref[0] >> 2) & 1


def pair_body(me_ref, own_ref, other_ref, full_ref, piece_ref, hi_ref, lo_ref, vec_ref):
    def go(first, second):
        both = mm(split(first[...]), split(second[:N, :]))
        vec = both[N:] + second[N:, :]
        hi_ref[...], lo_ref[...] = split(both[:N])
        full_ref[:N, :] = both[:N]
        full_ref[N:, :] = vec
        vec_ref[...] = vec

    @pl.when(core_of(me_ref) == 0)
    def _():
        go(own_ref, other_ref)

    @pl.when(core_of(me_ref) == 1)
    def _():
        go(other_ref, own_ref)

    piece_ref[:Q, :] = full_ref[pl.ds((me_ref[0] & 3) * Q, Q), :]
    piece_ref[Q:, :] = vec_ref[...]


def arrived(me_ref, value, news):
    for ref, chips in news:
        here = functools.reduce(jnp.logical_or, [(me_ref[0] >> 3) == chip for chip in chips])
        value = jnp.where(here, ref[...], value)
    return value


def hop_body(chip, me_ref, got_ref, had_ref, old_ref, hi_ref, lo_ref, vec_ref, in_ref, end_ref):
    here = (me_ref[0] >> 2) == 2 * chip + 1

    @pl.when(here)
    def _():
        in_ref[...] = got_ref[...]
        end_ref[...] = vec_ref[...] + mm(split(got_ref[...]), (hi_ref[...], lo_ref[...]))

    @pl.when(jnp.logical_not(here))
    def _():
        in_ref[...] = had_ref[...]
        end_ref[...] = old_ref[...]


def upper_only(me_ref):
    return (core_of(me_ref) == 1) & (me_ref[0] >= 32)


def pick_body(chips, me_ref, *refs):
    *news, out_ref = refs
    out_ref[...] = arrived(me_ref, jnp.zeros((R, N), F32), list(zip(news, chips)))


def near_body(me_ref, full_ref, hi_ref, lo_ref, vec_ref):
    @pl.when(upper_only(me_ref))
    def _():
        hi_ref[...], lo_ref[...] = split(full_ref[:N, :])
        vec_ref[...] = full_ref[N:, :]


def far_body(me_ref, *refs):
    quarter_ref, *pieces, hi_ref, lo_ref, vec_ref = refs

    @pl.when(upper_only(me_ref))
    def _():
        for s, piece in zip((0, 1, 3, 2), [quarter_ref, *pieces]):
            rows = pl.ds(((me_ref[0] + s) & 3) * Q, Q)
            hi_ref[rows, :], lo_ref[rows, :] = split(piece[:Q, :])
        vec_ref[...] = quarter_ref[Q:, :]


def line_body(which, chips, me_ref, *refs):
    maps, had_ref, news, (in_ref, end_ref) = refs[:12], refs[12], refs[13:-2], refs[-2:]
    inflow = arrived(me_ref, had_ref[...], list(zip(news, chips)))
    in_ref[...] = inflow
    for x in range(4):
        @pl.when((me_ref[0] >> 2) == 8 * which + 2 * x + 1)
        def _():
            current = inflow
            for chip in range(4):
                hi, lo, vec = maps[3 * ((chip - x) % 4):][:3]
                current = vec[...] + mm(split(current), (hi[...], lo[...]))
            end_ref[...] = current


def ahead_body(me_ref, *refs):
    maps, (hi_ref, lo_ref, vec_ref) = refs[:12], refs[12:]
    for z, x, count in [(2, x, 4) for x in range(4)] + [(3, x, x) for x in range(1, 4)]:
        @pl.when((me_ref[0] >> 2) == 8 * z + 2 * x + 1)
        def _():
            hi, lo, vec = (r[...] for r in maps[3 * (-x % 4):][:3])
            for chip in range(1, count):
                later = [r[...] for r in maps[3 * ((chip - x) % 4):][:3]]
                vec = later[2] + mm(split(vec), later[:2])
                hi, lo = split(mm((hi, lo), later[:2]))
            hi_ref[...], lo_ref[...], vec_ref[...] = hi, lo, vec


def cross_body(chips, me_ref, had_ref, *refs):
    *news, hi_ref, lo_ref, vec_ref, in_ref, end_ref = refs
    inflow = arrived(me_ref, had_ref[...], list(zip(news, chips)))
    in_ref[...] = inflow

    @pl.when(upper_only(me_ref) & ((me_ref[0] >> 5) == 2))
    def _():
        end_ref[...] = vec_ref[...] + mm(split(inflow), (hi_ref[...], lo_ref[...]))


def inner_body(me_ref, *refs):
    maps, had_ref, in_ref = refs[:12], refs[12], refs[13]
    line = me_ref[0] >> 5
    for x in range(4):
        @pl.when(upper_only(me_ref) & (line < 3) & (((me_ref[0] >> 3) & 3) == x))
        def _():
            current = had_ref[...]
            for chip in range(x):
                hi, lo, vec = maps[3 * ((chip - x) % 4):][:3]
                current = vec[...] + mm(split(current), (hi[...], lo[...]))
            in_ref[...] = current


def final_body(me_ref, ahead_hi_ref, ahead_lo_ref, ahead_vec_ref, walked_ref, inner_ref, got_ref, in_ref):
    line = me_ref[0] >> 5
    x = (me_ref[0] >> 3) & 3

    @pl.when(line == 0)
    def _():
        in_ref[...] = walked_ref[...]

    @pl.when((line == 1) | (line == 2))
    def _():
        in_ref[...] = inner_ref[...]

    @pl.when((line == 3) & (x == 0))
    def _():
        in_ref[...] = got_ref[...]

    @pl.when((line == 3) & (x > 0) & (core_of(me_ref) == 1))
    def _():
        in_ref[...] = ahead_vec_ref[...] + mm(split(got_ref[...]), (ahead_hi_ref[...], ahead_lo_ref[...]))


def last_body(me_ref, down_ref, in_ref, own_ref, hi_ref, lo_ref, vec_ref, walk_end_ref, out_ref):
    @pl.when(core_of(me_ref) == 0)
    def _():
        out_ref[...] = own_ref[N:, :] + mm(split(down_ref[...]), split(own_ref[:N, :]))

    @pl.when((core_of(me_ref) == 1) & (me_ref[0] < 32))
    def _():
        out_ref[...] = walk_end_ref[...]

    @pl.when(upper_only(me_ref))
    def _():
        out_ref[...] = vec_ref[...] + mm(split(in_ref[...]), (hi_ref[...], lo_ref[...]))


def kernel(body, outs, scratch=(), space=pltpu.VMEM):
    smem = pl.BlockSpec(memory_space=pltpu.SMEM)
    data = pl.BlockSpec(memory_space=space)

    def call(*args):
        args = [a if a.dtype == jnp.int32 else pltpu.with_memory_space_constraint(a, space) for a in args]
        return pl.pallas_call(
            body,
            out_shape=outs,
            in_specs=[smem if a.dtype == jnp.int32 else data for a in args],
            out_specs=jax.tree.map(lambda _: pl.BlockSpec(memory_space=pltpu.VMEM), outs),
            scratch_shapes=scratch,
            compiler_params=pltpu.CompilerParams(vmem_limit_bytes=16 << 20),
        )(*args)

    return call


def arr(rows, dtype=F32):
    return pltpu.VMEM((rows, N), dtype)


def device(z, x, core, y):
    return ((z * 4 + x) * 2 + core) * 4 + y


def complete(moves):
    pairs = dict(moves)
    taken = set(pairs.values())
    for source, target in list(pairs.items()):
        for a, b in ((target, target ^ 4), (target ^ 4, source ^ 4), (source ^ 4, source)):
            if a not in pairs and b not in taken:
                pairs[a] = b
                taken.add(b)
    for i in range(128):
        if i not in pairs:
            pairs[i] = i ^ 4
            taken.add(i ^ 4)
    assert len(taken) == 128 and all(a != b for a, b in pairs.items())
    return sorted(pairs.items())


def hops(pairs):
    return complete([(device(*a, 1, y), device(*b, 1, y)) for a, b in pairs for y in range(4)])


LINES = [(z, x, y) for z in range(1, 4) for x in range(4) for y in range(4)]


def ring(x_step, y_step):
    return [(device(z, (x + x_step) % 4, 1, (y + y_step) % 4), device(z, x, 1, y)) for z, x, y in LINES]


def full_ring(x_step, y_step):
    return complete(ring(x_step, y_step) + [(device(z, x, 0, y), device(z % 3 + 1, x, 0, y)) for z, x, y in LINES])


def local(diag_blocks, sub_blocks, right_side, boundary):
    def send(value, pairs):
        return lax.ppermute(value, ALL, pairs)

    me = lax.axis_index(ALL).astype(jnp.int32).reshape(1)
    loads = [
        pltpu.VMEM((1, N, N), F32), pltpu.VMEM((1, N, N), F32), pltpu.VMEM((R, N), F32),
        pltpu.VMEM((R, N), F32), pltpu.SemaphoreType.DMA((4,)),
    ]
    own = kernel(local_body, arr(N + R), loads, pltpu.HBM)(
        me, diag_blocks, sub_blocks, right_side, boundary.T)
    other = lax.ppermute(own, "c", [(0, 1), (1, 0)])
    weights, two = [arr(N, BF16), arr(N, BF16), arr(R)], [arr(R), arr(R)]
    full, piece, *here = kernel(pair_body, [arr(N + R), arr(Q + R)] + weights)(me, own, other)
    hi, lo, vec = here

    quarters = [send(piece, full_ring(2, 0))]
    left = send(full, ring(-1, 0))
    right = send(full, ring(1, 0))
    quarters += [send(quarters[0][:Q], full_ring(0, s)) for s in (1, 3, 2)]

    walked, walk_end = jnp.zeros((R, N), F32), vec
    for x in range(3):
        got = send(walk_end, hops([((0, x), (0, x + 1))]))
        hop = kernel(functools.partial(hop_body, x + 1), two)
        walked, walk_end = hop(me, got, walked, walk_end, hi, lo, vec)
    first = send(walk_end, hops([((0, 3), (1, 3))]))
    second = send(walk_end, hops([((0, 3), (1, 0))]))
    inflow = kernel(functools.partial(pick_body, [(7,), (4,)]), arr(R))(me, first, second)
    third = send(inflow, hops([((1, 3), (1, 2)), ((1, 0), (1, 1))]))

    far = kernel(far_body, weights)(me, *quarters)
    near = kernel(near_body, weights)
    maps = [*here, *near(me, right), *far, *near(me, left)]

    line = kernel(functools.partial(line_body, 1, [(5, 6)]), two)
    inflow, end = line(me, *maps, inflow, third)
    fourth = send(end, hops([((1, x), (2, x)) for x in range(4)]))
    ahead = kernel(ahead_body, weights)(me, *maps)
    cross = kernel(functools.partial(cross_body, [(8, 9, 10, 11)]), two)
    inflow, end = cross(me, inflow, fourth, *ahead)
    fifth = send(end, hops([((2, x), (3, x)) for x in range(4)]))
    inner = kernel(inner_body, arr(R))(me, *maps, inflow)
    inflow = kernel(final_body, arr(R))(me, *ahead, walked, inner, fifth)
    down = lax.ppermute(inflow, "c", [(0, 1), (1, 0)])
    return kernel(last_body, jax.ShapeDtypeStruct((R, N), F32))(
        me, down, inflow, own, hi, lo, vec, walk_end)


def solution(mesh):
    split_mesh = Mesh(mesh.devices.reshape(4, 4, 2, 4), ALL)
    placed = (P(SLAB, None, None), P(SLAB, None, None), P("y", SLAB), P(None, "y"))

    return jax.shard_map(local, mesh=split_mesh, in_specs=placed, out_specs=P("y", SLAB), check_vma=False)
```

```python
import functools

import jax
import jax.numpy as jnp
from jax import lax
from jax.experimental import pallas as pl
from jax.experimental.pallas import tpu as pltpu
from jax.sharding import Mesh
from jax.sharding import PartitionSpec as P


SLAB = ("z", "x", "c")
ALL = ("z", "x", "c", "y")
F32 = jnp.float32
BF16 = jnp.bfloat16
N = 512
H = 256
Q = 128
R = 64


def split(a):
    hi = a.astype(BF16)
    return hi, (a - hi.astype(F32)).astype(BF16)


def dot(a, b):
    return lax.dot_general(a, b, (((1,), (0,)), ((), ())), preferred_element_type=F32)


def mm(a, b):
    return dot(a[0], b[0]) + (dot(a[0], b[1]) + dot(a[1], b[0]))


def mm_small(a, b):
    ah, al = split(a)
    bh, bl = split(b)
    row = jnp.concatenate([bh, bl], axis=1)
    both = dot(jnp.concatenate([ah, al], axis=1), jnp.concatenate([row, row], axis=0))
    return both[:, :Q] + both[:, Q:]


def local_body(me_ref, diag_hbm, sub_hbm, right_hbm, bound_hbm, out_ref, diag_ref, sub_ref, right_ref, bound_ref, ups_ref, sems):
    loads = [
        pltpu.make_async_copy(src, dst, sems.at[i])
        for i, (src, dst) in enumerate([
            (diag_hbm, diag_ref), (sub_hbm, sub_ref), (right_hbm, right_ref), (bound_hbm, bound_ref)])
    ]
    spans = [slice(i * Q, (i + 1) * Q) for i in range(4)]
    blocks = [pltpu.make_async_copy(diag_hbm.at[0, r, r], ups_ref.at[i], sems.at[4 + i]) for i, r in enumerate(spans)]
    for load in blocks + loads:
        load.start()
    for load in blocks:
        load.wait()
    row = lax.broadcasted_iota(jnp.int32, (Q, Q), 0)
    col = lax.broadcasted_iota(jnp.int32, (Q, Q), 1)
    eye = row == col

    def block(i, j):
        return diag_ref[0, j * Q:(j + 1) * Q, i * Q:(i + 1) * Q].T

    ups = [ups_ref[i].T for i in range(4)]
    inv = []
    for u in ups:
        d = jnp.where(eye, u, 0.0)
        across = 1.0 / jnp.sum(d, axis=0, keepdims=True)
        down = 1.0 / jnp.sum(d, axis=1, keepdims=True)
        pair = ((row & 1) == 0) & (col == row + 1)
        inv.append(jnp.where(eye, across, jnp.where(pair, -(down * u) * across, 0.0)))
    for level in range(1, 7):
        rb, cb = row >> level, col >> level
        pick = ((rb & 1) == 0) & (cb == rb + 1)
        half = [mm_small(x, jnp.where(pick, u, 0.0)) for x, u in zip(inv, ups)]
        inv = [x - mm_small(h, x) for h, x in zip(half, inv)]
    loads[0].wait()
    tiles = []
    for i in (0, 2):
        off = mm_small(mm_small(inv[i], block(i, i + 1)), inv[i + 1])
        zero = jnp.zeros((Q, Q), F32)
        tiles.append(split(jnp.concatenate([
            jnp.concatenate([inv[i], -off], axis=1),
            jnp.concatenate([zero, inv[i + 1]], axis=1)], axis=0)))
    for load in loads[1:]:
        load.wait()
    left0 = jnp.concatenate([sub_ref[0, :H, :].T, right_ref[:, :H]], axis=0)
    right0 = jnp.concatenate([sub_ref[0, H:, :].T, right_ref[:, H:]], axis=0)
    left = mm(split(left0), tiles[0])
    cross = split(diag_ref[0, H:, :H].T)
    right = mm(split(right0 - mm(split(left), cross)), tiles[1])
    out_ref[:N, :H] = -left[:N]
    out_ref[:N, H:] = -right[:N]
    out_ref[N:, :H] = left[N:]
    out_ref[N:, H:] = right[N:]

    @pl.when(me_ref[0] < 4)
    def _():
        out_ref[N:, :] += mm(split(bound_ref[...]), split(out_ref[:N, :]))


def core_of(me_ref):
    return (me_ref[0] >> 2) & 1


def pair_body(me_ref, own_ref, other_ref, full_ref, piece_ref, hi_ref, lo_ref, vec_ref):
    def go(first, second):
        both = mm(split(first[...]), split(second[:N, :]))
        vec = both[N:] + second[N:, :]
        hi_ref[...], lo_ref[...] = split(both[:N])
        full_ref[:N, :] = both[:N]
        full_ref[N:, :] = vec
        vec_ref[...] = vec

    @pl.when(core_of(me_ref) == 1)
    def _():
        go(other_ref, own_ref)

    piece_ref[:Q, :] = full_ref[pl.ds((me_ref[0] & 3) * Q, Q), :]
    piece_ref[Q:, :] = vec_ref[...]


def arrived(me_ref, value, news):
    for ref, chips in news:
        here = functools.reduce(jnp.logical_or, [(me_ref[0] >> 3) == chip for chip in chips])
        value = jnp.where(here, ref[...], value)
    return value


def hop_body(chip, me_ref, got_ref, had_ref, old_ref, hi_ref, lo_ref, vec_ref, in_ref, end_ref):
    here = (me_ref[0] >> 2) == 2 * chip + 1

    @pl.when(here)
    def _():
        in_ref[...] = got_ref[...]
        end_ref[...] = vec_ref[...] + mm(split(got_ref[...]), (hi_ref[...], lo_ref[...]))

    @pl.when(jnp.logical_not(here))
    def _():
        in_ref[...] = had_ref[...]
        end_ref[...] = old_ref[...]


def upper_only(me_ref):
    return (core_of(me_ref) == 1) & (me_ref[0] >= 32)


def pick_body(chips, me_ref, *refs):
    *news, out_ref = refs
    out_ref[...] = arrived(me_ref, jnp.zeros((R, N), F32), list(zip(news, chips)))


def near_body(me_ref, full_ref, hi_ref, lo_ref, vec_ref):
    @pl.when(upper_only(me_ref))
    def _():
        hi_ref[...], lo_ref[...] = split(full_ref[:N, :])
        vec_ref[...] = full_ref[N:, :]


def far_body(me_ref, *refs):
    quarter_ref, *pieces, hi_ref, lo_ref, vec_ref = refs

    @pl.when(upper_only(me_ref))
    def _():
        for s, piece in zip((0, 1, 3, 2), [quarter_ref, *pieces]):
            rows = pl.ds(((me_ref[0] + s) & 3) * Q, Q)
            hi_ref[rows, :], lo_ref[rows, :] = split(piece[:Q, :])
        vec_ref[...] = quarter_ref[Q:, :]


def line_body(which, chips, me_ref, *refs):
    maps, had_ref, news, (in_ref, end_ref) = refs[:12], refs[12], refs[13:-2], refs[-2:]
    inflow = arrived(me_ref, had_ref[...], list(zip(news, chips)))
    in_ref[...] = inflow
    for x in range(4):
        @pl.when((me_ref[0] >> 2) == 8 * which + 2 * x + 1)
        def _():
            current = inflow
            for chip in range(4):
                hi, lo, vec = maps[3 * ((chip - x) % 4):][:3]
                current = vec[...] + mm(split(current), (hi[...], lo[...]))
            end_ref[...] = current


def ahead_body(me_ref, *refs):
    maps, (hi_ref, lo_ref, vec_ref) = refs[:12], refs[12:]
    for z, x, count in [(2, x, 4) for x in range(4)] + [(3, x, x) for x in range(1, 4)]:
        @pl.when((me_ref[0] >> 2) == 8 * z + 2 * x + 1)
        def _():
            hi, lo, vec = (r[...] for r in maps[3 * (-x % 4):][:3])
            for chip in range(1, count):
                later = [r[...] for r in maps[3 * ((chip - x) % 4):][:3]]
                vec = later[2] + mm(split(vec), later[:2])
                hi, lo = split(mm((hi, lo), later[:2]))
            hi_ref[...], lo_ref[...], vec_ref[...] = hi, lo, vec


def cross_body(chips, me_ref, had_ref, *refs):
    *news, hi_ref, lo_ref, vec_ref, in_ref, end_ref = refs
    inflow = arrived(me_ref, had_ref[...], list(zip(news, chips)))
    in_ref[...] = inflow

    @pl.when(upper_only(me_ref) & ((me_ref[0] >> 5) == 2))
    def _():
        end_ref[...] = vec_ref[...] + mm(split(inflow), (hi_ref[...], lo_ref[...]))


def inner_body(me_ref, *refs):
    maps, had_ref, in_ref = refs[:12], refs[12], refs[13]
    line = me_ref[0] >> 5
    for x in range(4):
        @pl.when(upper_only(me_ref) & (line < 3) & (((me_ref[0] >> 3) & 3) == x))
        def _():
            current = had_ref[...]
            for chip in range(x):
                hi, lo, vec = maps[3 * ((chip - x) % 4):][:3]
                current = vec[...] + mm(split(current), (hi[...], lo[...]))
            in_ref[...] = current


def final_body(me_ref, ahead_hi_ref, ahead_lo_ref, ahead_vec_ref, walked_ref, inner_ref, got_ref, in_ref):
    line = me_ref[0] >> 5
    x = (me_ref[0] >> 3) & 3

    @pl.when(line == 0)
    def _():
        in_ref[...] = walked_ref[...]

    @pl.when((line == 1) | (line == 2))
    def _():
        in_ref[...] = inner_ref[...]

    @pl.when((line == 3) & (x == 0))
    def _():
        in_ref[...] = got_ref[...]

    @pl.when((line == 3) & (x > 0) & (core_of(me_ref) == 1))
    def _():
        in_ref[...] = ahead_vec_ref[...] + mm(split(got_ref[...]), (ahead_hi_ref[...], ahead_lo_ref[...]))


def last_body(me_ref, down_ref, in_ref, own_ref, hi_ref, lo_ref, vec_ref, walk_end_ref, out_ref):
    @pl.when(core_of(me_ref) == 0)
    def _():
        out_ref[...] = own_ref[N:, :] + mm(split(down_ref[...]), split(own_ref[:N, :]))

    @pl.when((core_of(me_ref) == 1) & (me_ref[0] < 32))
    def _():
        out_ref[...] = walk_end_ref[...]

    @pl.when(upper_only(me_ref))
    def _():
        out_ref[...] = vec_ref[...] + mm(split(in_ref[...]), (hi_ref[...], lo_ref[...]))


def kernel(body, outs, scratch=(), space=pltpu.VMEM):
    smem = pl.BlockSpec(memory_space=pltpu.SMEM)
    data = pl.BlockSpec(memory_space=space)

    def call(*args):
        args = [a if a.dtype == jnp.int32 else pltpu.with_memory_space_constraint(a, space) for a in args]
        return pl.pallas_call(
            body,
            out_shape=outs,
            in_specs=[smem if a.dtype == jnp.int32 else data for a in args],
            out_specs=jax.tree.map(lambda _: pl.BlockSpec(memory_space=pltpu.VMEM), outs),
            scratch_shapes=scratch,
            compiler_params=pltpu.CompilerParams(vmem_limit_bytes=16 << 20),
        )(*args)

    return call


def arr(rows, dtype=F32):
    return pltpu.VMEM((rows, N), dtype)


def device(z, x, core, y):
    return ((z * 4 + x) * 2 + core) * 4 + y


def complete(moves):
    pairs = dict(moves)
    taken = set(pairs.values())
    for source, target in list(pairs.items()):
        for a, b in ((target, target ^ 4), (target ^ 4, source ^ 4), (source ^ 4, source)):
            if a not in pairs and b not in taken:
                pairs[a] = b
                taken.add(b)
    for i in range(128):
        if i not in pairs:
            pairs[i] = i ^ 4
            taken.add(i ^ 4)
    assert len(taken) == 128 and all(a != b for a, b in pairs.items())
    return sorted(pairs.items())


def hops(pairs):
    return complete([(device(*a, 1, y), device(*b, 1, y)) for a, b in pairs for y in range(4)])


LINES = [(z, x, y) for z in range(1, 4) for x in range(4) for y in range(4)]


def ring(x_step, y_step):
    return [(device(z, (x + x_step) % 4, 1, (y + y_step) % 4), device(z, x, 1, y)) for z, x, y in LINES]


def full_ring(x_step, y_step):
    return complete(ring(x_step, y_step) + [(device(z, x, 0, y), device(z % 3 + 1, x, 0, y)) for z, x, y in LINES])


def local(diag_blocks, sub_blocks, right_side, boundary):
    def send(value, pairs):
        return lax.ppermute(value, ALL, pairs)

    me = lax.axis_index(ALL).astype(jnp.int32).reshape(1)
    loads = [
        pltpu.VMEM((1, N, N), F32), pltpu.VMEM((1, N, N), F32), pltpu.VMEM((R, N), F32),
        pltpu.VMEM((R, N), F32), pltpu.VMEM((4, Q, Q), F32), pltpu.SemaphoreType.DMA((8,)),
    ]
    own = kernel(local_body, arr(N + R), loads, pltpu.HBM)(
        me, diag_blocks, sub_blocks, right_side, boundary.T)
    other = lax.ppermute(own, "c", [(0, 1), (1, 0)])
    weights, two = [arr(N, BF16), arr(N, BF16), arr(R)], [arr(R), arr(R)]
    full, piece, *here = kernel(pair_body, [arr(N + R), arr(Q + R)] + weights)(me, own, other)
    hi, lo, vec = here

    quarters = [send(piece, full_ring(2, 0))]
    left = send(full, ring(-1, 0))
    right = send(full, ring(1, 0))
    quarters += [send(quarters[0][:Q], full_ring(0, s)) for s in (1, 3, 2)]

    walked, walk_end = jnp.zeros((R, N), F32), vec
    for x in range(3):
        got = send(walk_end, hops([((0, x), (0, x + 1))]))
        hop = kernel(functools.partial(hop_body, x + 1), two)
        walked, walk_end = hop(me, got, walked, walk_end, hi, lo, vec)
    first = send(walk_end, hops([((0, 3), (1, 3))]))
    second = send(walk_end, hops([((0, 3), (1, 0))]))
    inflow = kernel(functools.partial(pick_body, [(7,), (4,)]), arr(R))(me, first, second)
    third = send(inflow, hops([((1, 3), (1, 2)), ((1, 0), (1, 1))]))

    far = kernel(far_body, weights)(me, *quarters)
    near = kernel(near_body, weights)
    maps = [*here, *near(me, right), *far, *near(me, left)]

    line = kernel(functools.partial(line_body, 1, [(5, 6)]), two)
    inflow, end = line(me, *maps, inflow, third)
    fourth = send(end, hops([((1, x), (2, x)) for x in range(4)]))
    ahead = kernel(ahead_body, weights)(me, *maps)
    cross = kernel(functools.partial(cross_body, [(8, 9, 10, 11)]), two)
    inflow, end = cross(me, inflow, fourth, *ahead)
    fifth = send(end, hops([((2, x), (3, x)) for x in range(4)]))
    inner = kernel(inner_body, arr(R))(me, *maps, inflow)
    inflow = kernel(final_body, arr(R))(me, *ahead, walked, inner, fifth)
    down = lax.ppermute(inflow, "c", [(0, 1), (1, 0)])
    return kernel(last_body, jax.ShapeDtypeStruct((R, N), F32))(
        me, down, inflow, own, hi, lo, vec, walk_end)


def solution(mesh):
    split_mesh = Mesh(mesh.devices.reshape(4, 4, 2, 4), ALL)
    placed = (P(SLAB, None, None), P(SLAB, None, None), P("y", SLAB), P(None, "y"))

    return jax.shard_map(local, mesh=split_mesh, in_specs=placed, out_specs=P("y", SLAB), check_vma=False)
```
